32 devices in a mesh: dp: 8 (over z, y), head: 4 (over x, core).
Axes of the slice: x: 2, y: 2, z: 4, core: 2. Of those that a mesh axis runs over, the one named last changes fastest.
Arguments:
- tokens: bfloat16 [3, 8192, 768], P(None, ('dp', 'head')), may hold values from -6 to 6
- cotangent: bfloat16 [3, 8192, 768], P(None, ('dp', 'head')), may hold values from -6 to 6
- bucket_ids: int32 [3, 16], P(None, 'dp'), may hold values from 0 to 2, as said below
- seq_lengths: int32 [3, 16, 8], P(None, 'dp'), may hold values from 0 to 256, as said below
- query_weight: bfloat16 [768, 768], P('dp', 'head'), may hold values from -0.3125 to 0.3125
- query_bias: bfloat16 [12, 64], P('head', 'dp'), may hold values from -3 to 3
- key_weight: bfloat16 [768, 768], P('dp', 'head'), may hold values from -0.21875 to 0.21875
- value_weight: bfloat16 [768, 768], P('dp', 'head'), may hold values from -0.21875 to 0.21875
- value_bias: bfloat16 [12, 64], P('head', 'dp'), may hold values from -3 to 3
- output_weight: bfloat16 [768, 768], P(('dp', 'head')), may hold values from -0.875 to 0.875
- output_bias: bfloat16 [768], P(('dp', 'head')), may hold values from -3 to 3
- first_gain: bfloat16 [768], P(('dp', 'head')), may hold values from 0.25 to 1.75
- first_shift: bfloat16 [768], P(('dp', 'head')), may hold values from -3 to 3
- inner_weight: bfloat16 [768, 3072], P(('dp', 'head')), may hold values from -0.21875 to 0.21875
- inner_bias: bfloat16 [3072], P(('dp', 'head')), may hold values from -3 to 3
- outer_weight: bfloat16 [3072, 768], P(('dp', 'head')), may hold values from -0.109375 to 0.109375
- outer_bias: bfloat16 [768], P(('dp', 'head')), may hold values from -3 to 3
- second_gain: bfloat16 [768], P(('dp', 'head')), may hold values from 0.25 to 1.75
- second_shift: bfloat16 [768], P(('dp', 'head')), may hold values from -3 to 3
Outputs:
- layer_out: bfloat16 [3, 8192, 768], P(None, ('dp', 'head'))
- input_grad: bfloat16 [3, 8192, 768], P(None, ('dp', 'head'))
- grad_query_weight: float32 [768, 768], P('dp', 'head')
- grad_query_bias: float32 [12, 64], P('head', 'dp')
- grad_key_weight: float32 [768, 768], P('dp', 'head')
- grad_value_weight: float32 [768, 768], P('dp', 'head')
- grad_value_bias: float32 [12, 64], P('head', 'dp')
- grad_output_weight: float32 [768, 768], P(('dp', 'head'))
- grad_output_bias: float32 [768], P(('dp', 'head'))
- grad_first_gain: float32 [768], P(('dp', 'head'))
- grad_first_shift: float32 [768], P(('dp', 'head'))
- grad_inner_weight: float32 [768, 3072], P(('dp', 'head'))
- grad_inner_bias: float32 [3072], P(('dp', 'head'))
- grad_outer_weight: float32 [3072, 768], P(('dp', 'head'))
- grad_outer_bias: float32 [768], P(('dp', 'head'))
- grad_second_gain: float32 [768], P(('dp', 'head'))
- grad_second_shift: float32 [768], P(('dp', 'head'))
The draws below stay inside these ranges and needn't reach their ends.
Inputs may be any that keep to these rules, and one draw needn't show every extreme that they name: `bucket_ids`: every micro-batch has some block of bucket 2 and some block of bucket 0; a block of bucket b holds 8 / 2^b sequences of 64 * 2^b rows each. `seq_lengths`: in a block of bucket b the first 8 / 2^b entries are lengths from 1 to 64 * 2^b and the others are 0; in every micro-batch some block holds a sequence of length 256.
All inputs are finite; a program needn't handle non-finite values.
Results may differ from the reference program's by a relative error of at most 0.017.
Values may be sent and summed in bfloat16 or wider, within the bound.
A program may use at most 128 MiB of HBM per device.

```python
import jax
import jax.numpy as jnp
from jax import lax

D = 768
HEADS = 12
HD = 64
FF = 3072
SHORT = 64
SLOTS = 8
MICRO = 3
BLOCK = 512
TOKENS = 8192
BLOCKS = 16


def draw_layout(key):
    bucket_key = jax.random.fold_in(key, 101)
    length_key = jax.random.fold_in(key, 202)
    choose_key = jax.random.fold_in(key, 303)
    buckets = jax.random.randint(bucket_key, (MICRO, BLOCKS), 0, 3)
    chosen = jax.random.randint(choose_key, (MICRO, 1), 0, BLOCKS)
    column = jnp.arange(BLOCKS)[None, :]
    buckets = jnp.where(column == chosen, 2, buckets)
    buckets = jnp.where(column == (chosen + 1) % BLOCKS, 0, buckets)
    seq_width = SHORT * jnp.where(buckets == 0, 1, jnp.where(buckets == 1, 2, 4))
    lengths = jax.random.randint(length_key, (MICRO, BLOCKS, SLOTS), 1, seq_width[:, :, None] + 1)
    per_block = SLOTS // (seq_width // SHORT)
    slot_index = jnp.arange(SLOTS)[None, None, :]
    lengths = jnp.where(slot_index < per_block[:, :, None], lengths, 0)
    lengths = jnp.where((column == chosen)[:, :, None] & (slot_index == 0), seq_width[:, :, None], lengths)
    return (buckets.astype(jnp.int32), lengths.astype(jnp.int32))


def draw_bucket_ids(key, part):
    return draw_layout(key)[0]


def draw_seq_lengths(key, part):
    return draw_layout(key)[1]


def strengthened(entries, rng, source, target, shards_of, factor):
    def block_of(axis_at):
        return (jnp.arange(entries.shape[axis_at]) // (entries.shape[axis_at] // shards_of)).reshape((-1,) + (1,) * (entries.ndim - 1 - axis_at))

    one_side = jax.random.permutation(rng, shards_of)[block_of(target)]
    other_side = (block_of(target) + shards_of // 2) % shards_of
    return jnp.where((block_of(source) == one_side) | (block_of(source) == other_side), factor * entries, entries)


def block_scale(rng, extent, cuts, least, top_value):
    gain = 1.0
    for dim, parts in cuts:
        draws = jax.random.uniform(jax.random.fold_in(jax.random.fold_in(rng, 6), dim), (parts,), jnp.float32, least / len(cuts), top_value / len(cuts))
        gain = gain * jnp.repeat(jnp.exp(draws), extent[dim] // parts).reshape((-1,) + (1,) * (len(extent) - 1 - dim))
    return gain


def noise(stream_key, dims, deviation, most, split=(), kind=jnp.bfloat16):
    values = jax.random.normal(stream_key, dims, jnp.float32) * deviation
    if len(split) > 0:
        values = block_scale(stream_key, dims, split, -0.22, 0.18) * values
    return jnp.clip(values, min=-most, max=most).astype(kind)


def heavy_noise(own_key, dims, scale, limit, pieces, heavy, kind=jnp.bfloat16):
    array = scale * jax.random.normal(own_key, dims, jnp.float32)
    if pieces:
        array = array * block_scale(own_key, dims, pieces, -0.22, 0.18)
    return jnp.clip(strengthened(array, jax.random.fold_in(own_key, 3), *heavy), -limit, limit).astype(kind)


def setup_inputs(seed: int = 0) -> dict:
    keys = jax.random.split(jax.random.key(seed), 20)
    tokens = heavy_noise(keys[0], (MICRO, TOKENS, D), 1.0, 6.0, ((1, 32),), (1, 2, 32, 2.75))
    cotangent = heavy_noise(keys[1], (MICRO, TOKENS, D), 1.0, 6.0, ((1, 32),), (1, 2, 32, 2.75))
    bucket_ids = draw_bucket_ids(jax.random.fold_in(keys[19], 71), 0)
    seq_lengths = draw_seq_lengths(jax.random.fold_in(keys[19], 71), 0)
    query_weight = noise(keys[4], (D, D), (D // 2) ** -0.5, 0.3125, ((0, 8), (1, 4)))
    query_bias = noise(keys[5], (HEADS, HD), 0.5, 3.0, ((0, 4), (1, 8)))
    key_weight = noise(keys[6], (D, D), D ** -0.5, 0.21875, ((0, 8), (1, 4)))
    value_weight = noise(keys[7], (D, D), D ** -0.5, 0.21875, ((0, 8), (1, 4)))
    value_bias = noise(keys[8], (HEADS, HD), 0.5, 3.0, ((0, 4), (1, 8)))
    output_weight = noise(keys[9], (D, D), (D // 16) ** -0.5, 0.875, ((0, 32),))
    output_bias = noise(keys[10], (D,), 0.5, 3.0, ((0, 32),))
    first_gain = jnp.clip(1.0 + 0.15 * jax.random.normal(keys[11], (D,), jnp.float32), 0.25, 1.75).astype(jnp.bfloat16)
    first_shift = noise(keys[12], (D,), 0.5, 3.0, ((0, 32),))
    inner_weight = noise(keys[13], (D, FF), D ** -0.5, 0.21875, ((0, 32),))
    inner_bias = noise(keys[14], (FF,), 0.5, 3.0, ((0, 32),))
    outer_weight = noise(keys[15], (FF, D), FF ** -0.5, 0.109375, ((0, 32),))
    outer_bias = noise(keys[16], (D,), 0.5, 3.0, ((0, 32),))
    second_gain = jnp.clip(1.0 + 0.15 * jax.random.normal(keys[17], (D,), jnp.float32), 0.25, 1.75).astype(jnp.bfloat16)
    second_shift = noise(keys[18], (D,), 0.5, 3.0, ((0, 32),))
    return dict(tokens=tokens, cotangent=cotangent, bucket_ids=bucket_ids, seq_lengths=seq_lengths, query_weight=query_weight, query_bias=query_bias, key_weight=key_weight, value_weight=value_weight, value_bias=value_bias, output_weight=output_weight, output_bias=output_bias, first_gain=first_gain, first_shift=first_shift, inner_weight=inner_weight, inner_bias=inner_bias, outer_weight=outer_weight, outer_bias=outer_bias, second_gain=second_gain, second_shift=second_shift)


@jax.custom_vjp
def low(v):
    return lax.optimization_barrier(v.astype(jnp.bfloat16)).astype(jnp.float32)

@jax.custom_vjp
def low_back(v):
    return v

def low_keep(v):
    return (low(v), None)

def low_pass(kept, grad):
    return (grad,)

def back_keep(v):
    return (v, None)

def back_low(kept, grad):
    return (low(grad),)
low.defvjp(low_keep, low_pass)
low_back.defvjp(back_keep, back_low)
highest_precision = lax.Precision.HIGHEST

def rounded_both(values):
    return low_back(low(values))

def product(left, right):
    return jnp.dot(left, right, precision=highest_precision, preferred_element_type=jnp.float32)

def gelu_erf(values):
    return 0.5 * values * (1.0 + lax.erf(values * 0.7071067811865476))

def layer_norm(values, gain_row, shift_row):
    centered = values - lax.optimization_barrier(jnp.mean(values, axis=-1, keepdims=True))
    variance = lax.optimization_barrier(jnp.mean(centered * centered, axis=-1, keepdims=True))
    return centered * lax.rsqrt(variance + 1e-12) * gain_row + shift_row

def block_mask(bucket, seq_lens):
    seq_width = SHORT * jnp.where(bucket == 0, 1, jnp.where(bucket == 1, 2, 4)).astype(jnp.int32)
    positions = jnp.arange(BLOCK, dtype=jnp.int32)
    member_seq = positions // seq_width
    within_seq = positions % seq_width
    lookup_table = (member_seq[:, None] == jnp.arange(SLOTS, dtype=jnp.int32)[None, :]).astype(jnp.int32)
    key_limit = lax.optimization_barrier(jnp.sum(lookup_table * seq_lens[None, :], axis=1))
    return (member_seq[:, None] == member_seq[None, :]) & (within_seq < key_limit)[None, :]

def attend_block(packed):
    query_blk, key_blk, value_blk, bucket, seq_lens = packed
    allowed = block_mask(bucket, seq_lens)
    scores = jnp.einsum('qhd,khd->hqk', query_blk, key_blk, precision=highest_precision) * HD ** (-0.5)
    scores = jnp.where(allowed[None], low_back(scores), -1e+30)
    row_top = lax.optimization_barrier(jnp.max(scores, axis=-1, keepdims=True))
    powered = jnp.exp(scores - row_top)
    softmax_out = powered / lax.optimization_barrier(jnp.sum(powered, axis=-1, keepdims=True))
    return jnp.einsum('hqk,khd->qhd', low(softmax_out), value_blk, precision=highest_precision)

def forward(tokens_in, layer_params, bucket_row, length_rows):
    query_weight, query_bias, key_weight, value_weight, value_bias, output_weight, output_bias, first_gain, first_shift, inner_weight, inner_bias, outer_weight, outer_bias, second_gain, second_shift = layer_params
    row_count = tokens_in.shape[0]
    flat_low = low(tokens_in)
    query_rows = rounded_both(product(flat_low, query_weight) + query_bias.reshape(-1))
    key_rows = rounded_both(product(flat_low, key_weight))
    value_rows = rounded_both(product(flat_low, value_weight) + value_bias.reshape(-1))
    block_shape = (row_count // BLOCK, BLOCK, HEADS, HD)
    attended = lax.map(jax.checkpoint(attend_block), (query_rows.reshape(block_shape), key_rows.reshape(block_shape), value_rows.reshape(block_shape), bucket_row, length_rows))
    mixed_rows = rounded_both(attended.reshape(row_count, D))
    branch_out = low_back(product(mixed_rows, output_weight) + output_bias)
    first_norm = layer_norm(tokens_in + branch_out, first_gain, first_shift)
    hidden_pre = low_back(product(low(first_norm), inner_weight) + inner_bias)
    active_low = low(gelu_erf(hidden_pre))
    outer_out = low_back(product(active_low, outer_weight) + outer_bias)
    return layer_norm(first_norm + outer_out, second_gain, second_shift)

def reference(tokens, cotangent, bucket_ids, seq_lengths, query_weight, query_bias, key_weight, value_weight, value_bias, output_weight, output_bias, first_gain, first_shift, inner_weight, inner_bias, outer_weight, outer_bias, second_gain, second_shift):
    params = tuple((weight.astype(jnp.float32) for weight in (query_weight, query_bias, key_weight, value_weight, value_bias, output_weight, output_bias, first_gain, first_shift, inner_weight, inner_bias, outer_weight, outer_bias, second_gain, second_shift)))
    outputs = []
    input_grads = []
    totals = None
    for micro_step in range(MICRO):

        def apply_layer(tokens_in, *layer_params):
            return forward(tokens_in, layer_params, bucket_ids[micro_step], seq_lengths[micro_step])
        result, pullback = jax.vjp(apply_layer, tokens[micro_step].astype(jnp.float32), *params)
        pulled = pullback(cotangent[micro_step].astype(jnp.float32))
        outputs.append(result.astype(jnp.bfloat16))
        input_grads.append(pulled[0].astype(jnp.bfloat16))
        if totals is None:
            totals = tuple(pulled[1:])
        else:
            totals = tuple((summed + addend for summed, addend in zip(totals, pulled[1:])))
    return (jnp.stack(outputs), jnp.stack(input_grads), totals[0], totals[1], totals[2], totals[3], totals[4], totals[5], totals[6], totals[7], totals[8], totals[9], totals[10], totals[11], totals[12], totals[13], totals[14])
```

```python
import jax
import jax.numpy as jnp
from jax import lax
from jax.sharding import PartitionSpec as P

HD = 64
SHORT = 64
SLOTS = 8
BLOCK = 512
LONGEST = 256

NEG_FILL = -1e30
SQRT_HALF = 0.7071067811865476
INV_SQRT_TAU = 0.3989422804014327
F32 = jnp.float32
BF16 = jnp.bfloat16


def norm_forward(values):
    centered = values - jnp.mean(values, axis=-1, keepdims=True)
    inverse_scale = lax.rsqrt(jnp.mean(centered * centered, axis=-1, keepdims=True) + 1e-12)
    return centered * inverse_scale, inverse_scale


def norm_backward(grad_out, normed, inverse_scale, gain_row):
    scaled = grad_out * gain_row
    return inverse_scale * (
        scaled
        - jnp.mean(scaled, axis=-1, keepdims=True)
        - normed * jnp.mean(scaled * normed, axis=-1, keepdims=True)
    )


def local_mask(bucket_ids, seq_lengths, rows):
    start = lax.axis_index("head") * rows
    block = start // BLOCK
    bucket = lax.dynamic_index_in_dim(bucket_ids, block, axis=1, keepdims=True)
    lens = lax.dynamic_index_in_dim(seq_lengths, block, axis=1, keepdims=False)
    width = SHORT * jnp.where(bucket == 0, 1, jnp.where(bucket == 1, 2, 4)).astype(jnp.int32)
    place = start % BLOCK + jnp.arange(rows, dtype=jnp.int32)[None, :]
    member = place // width
    within = place % width
    hit = (member[:, :, None] == jnp.arange(SLOTS, dtype=jnp.int32)[None, None, :]).astype(jnp.int32)
    limit = jnp.sum(hit * lens[:, None, :], axis=2)
    return (member[:, :, None] == member[:, None, :]) & (within < limit)[:, None, :]


def mm(a, b):
    return jnp.dot(a, b, preferred_element_type=F32)


def mm_nt(a, b):
    return lax.dot_general(a, b, (((1,), (1,)), ((), ())), preferred_element_type=F32)


def mm_tn(a, b):
    return lax.dot_general(a, b, (((0,), (0,)), ((), ())), preferred_element_type=F32)


def layer(x, dy, mask, p):
    micro, rows, width = x.shape
    heads = width // HD
    n = micro * rows
    x = x.reshape(n, width)
    dy = dy.reshape(n, width).astype(F32)
    (wq, qb, wk, wv, vb, wo, ob, g1, s1, wi, ib, wu, ub, g2, s2) = p
    f = lambda v: v.reshape(1, -1).astype(F32)
    shape = (micro, rows, heads, HD)
    q = (mm(x, wq) + f(qb)).astype(BF16).reshape(shape)
    k = mm(x, wk).astype(BF16).reshape(shape)
    v = (mm(x, wv) + f(vb)).astype(BF16).reshape(shape)
    scores = jnp.einsum("mqhd,mkhd->mhqk", q, k, preferred_element_type=F32) * HD**-0.5
    scores = jnp.where(mask[:, None], scores, NEG_FILL)
    top = jnp.max(scores, axis=-1, keepdims=True)
    powered = jnp.exp(scores - top)
    probs = powered / jnp.sum(powered, axis=-1, keepdims=True)
    att = jnp.einsum("mhqk,mkhd->mqhd", probs.astype(BF16), v, preferred_element_type=F32)
    att = att.astype(BF16).reshape(n, width)
    z1, q1 = norm_forward(x.astype(F32) + mm(att, wo) + f(ob))
    first = z1 * f(g1) + f(s1)
    first_low = first.astype(BF16)
    pre = mm(first_low, wi) + f(ib)
    cdf = 0.5 * (1.0 + lax.erf(pre * SQRT_HALF))
    active = (pre * cdf).astype(BF16)
    z2, q2 = norm_forward(first + mm(active, wu) + f(ub))
    out = (z2 * f(g2) + f(s2)).astype(BF16)
    g_second = norm_backward(dy, z2, q2, f(g2))
    g_outer = g_second.astype(BF16)
    slope = cdf + pre * INV_SQRT_TAU * jnp.exp(-0.5 * pre * pre)
    g_hidden = (mm_nt(g_outer, wu) * slope).astype(BF16)
    g_first = g_second + mm_nt(g_hidden, wi)
    g_branch = norm_backward(g_first, z1, q1, f(g1))
    g_branch_low = g_branch.astype(BF16)
    g_att = mm_nt(g_branch_low, wo).astype(BF16).reshape(shape)
    dprobs = jnp.einsum("mqhd,mkhd->mhqk", g_att, v, preferred_element_type=F32)
    inner = jnp.sum(dprobs * probs, axis=-1, keepdims=True)
    ds = (probs * (dprobs - inner)).astype(BF16)
    scale = HD**-0.5
    gq = (jnp.einsum("mhqk,mkhd->mqhd", ds, k, preferred_element_type=F32) * scale).astype(BF16)
    gk = (jnp.einsum("mhqk,mqhd->mkhd", ds, q, preferred_element_type=F32) * scale).astype(BF16)
    gv = jnp.einsum("mhqk,mqhd->mkhd", probs.astype(BF16), g_att, preferred_element_type=F32).astype(BF16)
    gq, gk, gv = (g.reshape(n, width) for g in (gq, gk, gv))
    g_in = (g_branch + mm_nt(gq, wq) + mm_nt(gk, wk) + mm_nt(gv, wv)).astype(BF16)
    rs = lambda g: jnp.sum(g.astype(F32), axis=0)
    big = (mm_tn(x, gq), mm_tn(x, gk), mm_tn(x, gv), mm_tn(att, g_branch_low), mm_tn(first_low, g_hidden), mm_tn(active, g_outer))
    small = (rs(gq), rs(gv), rs(g_branch_low), rs(g_first * z1), rs(g_first), rs(g_hidden), rs(g_outer), rs(dy * z2), rs(dy))
    return out.reshape(micro, rows, width), g_in.reshape(micro, rows, width), big, small


def body(tokens, cotangent, bucket_ids, seq_lengths, wq, qb, wk, wv, vb, wo, ob, g1, s1, wi, ib, wu, ub, g2, s2):
    both = ("dp", "head")
    rows = tokens.shape[1]
    assert rows % LONGEST == 0
    ag = lambda a, ax, dim: lax.all_gather(a, ax, axis=dim, tiled=True)
    n_head = lax.axis_size("head")
    wqkv = ag(jnp.stack([wq, wk, wv]), "dp", 1)
    wqkv = ag(wqkv, "head", 2)
    ob_, g1_, s1_, ub_, g2_, s2_, ib_ = (ag(a, both, 0) for a in (ob, g1, s1, ub, g2, s2, ib))
    qb_, vb_ = (ag(ag(a, "dp", 1), "head", 0) for a in (qb, vb))
    p = (wqkv[0], qb_, wqkv[1], wqkv[2], vb_, ag(wo, both, 0), ob_, g1_, s1_, ag(wi, both, 0), ib_, ag(wu, both, 0), ub_, g2_, s2_)
    mask = local_mask(bucket_ids, seq_lengths, rows)
    out, g_in, big, small = layer(tokens, cotangent, mask, p)
    sc = lambda a, ax, dim: lax.psum_scatter(a, ax, scatter_dimension=dim, tiled=True)
    gqkv = jnp.stack([b.astype(BF16) for b in big[:3]])
    gqkv = sc(sc(gqkv, "head", 2), "dp", 1).astype(F32)
    go, gi, gu = (sc(b.astype(BF16), both, 0).astype(F32) for b in big[3:])
    hb = lambda a: sc(sc(a.reshape(-1, HD), "head", 0), "dp", 1)
    s = small
    return (out, g_in, gqkv[0], hb(s[0]), gqkv[1], gqkv[2], hb(s[1]), go, sc(s[2], both, 0), sc(s[3], both, 0), sc(s[4], both, 0), gi, sc(s[5], both, 0), gu, sc(s[6], both, 0), sc(s[7], both, 0), sc(s[8], both, 0))


def solution(mesh):
    rows = P(None, ("dp", "head"), None)
    dense = P(("dp", "head"), None)
    flat = P(("dp", "head"))
    tile = P("dp", "head")
    bias = P("head", "dp")
    params = (tile, bias, tile, tile, bias, dense, flat, flat, flat, dense, flat, dense, flat, flat, flat)
    return jax.shard_map(
        body,
        mesh=mesh,
        in_specs=(rows, rows, P(None, "dp"), P(None, "dp", None)) + params,
        out_specs=(rows, rows) + params,
        check_vma=False,
    )
```

```python
import functools

import jax
import jax.numpy as jnp
from jax import lax
from jax.experimental import pallas as pl
from jax.experimental.pallas import tpu as pltpu
from jax.sharding import PartitionSpec as P

HD = 64
SHORT = 64
SLOTS = 8
BLOCK = 512
LONGEST = 256

NEG_FILL = -1e30
SQRT_HALF = 0.7071067811865476
INV_SQRT_TAU = 0.3989422804014327
F32 = jnp.float32
BF16 = jnp.bfloat16


def norm_forward(values):
    centered = values - jnp.mean(values, axis=-1, keepdims=True)
    inverse_scale = lax.rsqrt(jnp.mean(centered * centered, axis=-1, keepdims=True) + 1e-12)
    return centered * inverse_scale, inverse_scale


def norm_backward(grad_out, normed, inverse_scale, gain_row):
    scaled = grad_out * gain_row
    return inverse_scale * (
        scaled
        - jnp.mean(scaled, axis=-1, keepdims=True)
        - normed * jnp.mean(scaled * normed, axis=-1, keepdims=True)
    )


def local_mask(bucket_ids, seq_lengths, rows):
    start = lax.axis_index("head") * rows
    block = start // BLOCK
    bucket = lax.dynamic_index_in_dim(bucket_ids, block, axis=1, keepdims=True)
    lens = lax.dynamic_index_in_dim(seq_lengths, block, axis=1, keepdims=False)
    width = SHORT * jnp.where(bucket == 0, 1, jnp.where(bucket == 1, 2, 4)).astype(jnp.int32)
    place = start % BLOCK + jnp.arange(rows, dtype=jnp.int32)[None, :]
    member = place // width
    within = place % width
    hit = (member[:, :, None] == jnp.arange(SLOTS, dtype=jnp.int32)[None, None, :]).astype(jnp.int32)
    limit = jnp.sum(hit * lens[:, None, :], axis=2)
    return (member[:, :, None] == member[:, None, :]) & (within < limit)[:, None, :]


def mm(a, b):
    return jnp.dot(a, b, preferred_element_type=F32)


def mm_nt(a, b):
    return lax.dot_general(a, b, (((1,), (1,)), ((), ())), preferred_element_type=F32)


def mm_tn(a, b):
    return lax.dot_general(a, b, (((0,), (0,)), ((), ())), preferred_element_type=F32)


def layer(x, dy, mask, p):
    micro, rows, width = x.shape
    heads = width // HD
    n = micro * rows
    x = x.reshape(n, width)
    dy = dy.reshape(n, width).astype(F32)
    (wq, qb, wk, wv, vb, wo, ob, g1, s1, wi, ib, wu, ub, g2, s2) = p
    f = lambda v: v.reshape(1, -1).astype(F32)
    shape = (micro, rows, heads, HD)
    q = (mm(x, wq) + f(qb)).astype(BF16).reshape(shape)
    k = mm(x, wk).astype(BF16).reshape(shape)
    v = (mm(x, wv) + f(vb)).astype(BF16).reshape(shape)
    scores = jnp.einsum("mqhd,mkhd->mhqk", q, k, preferred_element_type=F32) * HD**-0.5
    scores = jnp.where(mask[:, None], scores, NEG_FILL)
    top = jnp.max(scores, axis=-1, keepdims=True)
    powered = jnp.exp(scores - top)
    probs = powered / jnp.sum(powered, axis=-1, keepdims=True)
    att = jnp.einsum("mhqk,mkhd->mqhd", probs.astype(BF16), v, preferred_element_type=F32)
    att = att.astype(BF16).reshape(n, width)
    z1, q1 = norm_forward(x.astype(F32) + mm(att, wo) + f(ob))
    first = z1 * f(g1) + f(s1)
    first_low = first.astype(BF16)
    pre = mm(first_low, wi) + f(ib)
    cdf = 0.5 * (1.0 + lax.erf(pre * SQRT_HALF))
    active = (pre * cdf).astype(BF16)
    z2, q2 = norm_forward(first + mm(active, wu) + f(ub))
    out = (z2 * f(g2) + f(s2)).astype(BF16)
    g_second = norm_backward(dy, z2, q2, f(g2))
    g_outer = g_second.astype(BF16)
    slope = cdf + pre * INV_SQRT_TAU * jnp.exp(-0.5 * pre * pre)
    g_hidden = (mm_nt(g_outer, wu) * slope).astype(BF16)
    g_first = g_second + mm_nt(g_hidden, wi)
    g_branch = norm_backward(g_first, z1, q1, f(g1))
    g_branch_low = g_branch.astype(BF16)
    g_att = mm_nt(g_branch_low, wo).astype(BF16).reshape(shape)
    dprobs = jnp.einsum("mqhd,mkhd->mhqk", g_att, v, preferred_element_type=F32)
    inner = jnp.sum(dprobs * probs, axis=-1, keepdims=True)
    ds = (probs * (dprobs - inner)).astype(BF16)
    scale = HD**-0.5
    gq = (jnp.einsum("mhqk,mkhd->mqhd", ds, k, preferred_element_type=F32) * scale).astype(BF16)
    gk = (jnp.einsum("mhqk,mqhd->mkhd", ds, q, preferred_element_type=F32) * scale).astype(BF16)
    gv = jnp.einsum("mhqk,mqhd->mkhd", probs.astype(BF16), g_att, preferred_element_type=F32).astype(BF16)
    gq, gk, gv = (g.reshape(n, width) for g in (gq, gk, gv))
    g_in = (g_branch + mm_nt(gq, wq) + mm_nt(gk, wk) + mm_nt(gv, wv)).astype(BF16)
    rs = lambda g: jnp.sum(g.astype(F32), axis=0)
    big = (mm_tn(x, gq), mm_tn(x, gk), mm_tn(x, gv), mm_tn(att, g_branch_low), mm_tn(first_low, g_hidden), mm_tn(active, g_outer))
    small = (rs(gq), rs(gv), rs(g_branch_low), rs(g_first * z1), rs(g_first), rs(g_hidden), rs(g_outer), rs(dy * z2), rs(dy))
    return out.reshape(micro, rows, width), g_in.reshape(micro, rows, width), big, small


def flipped(j, n_dp, n_head):
    def one(me, bits):
        out = me
        w = 1
        while w <= bits:
            if bits & w:
                out = out + w * (1 - 2 * lax.rem(lax.div(me, w), 2))
            w *= 2
        return out

    return one(lax.axis_index("dp"), j // n_head), one(lax.axis_index("head"), j % n_head)


def link_orders(n):
    bits = [1 << b for b in range(n.bit_length() - 2, 0, -1)]
    if len(bits) == 4:
        zh, zl, y, x = bits
        return ((zh, zl, y, x), (zh, zl, x, y), (x, zh, zl, y), (zh, zl, y, x))
    return (tuple(bits),) * 4


def greet(n, n_dp, n_head):
    barrier = pltpu.get_barrier_semaphore()
    count = 0
    b = 1
    while b < n:
        pl.semaphore_signal(barrier, inc=1, device_id=flipped(b, n_dp, n_head), device_id_type=pl.DeviceIdType.MESH)
        count += 1
        b *= 2
    pl.semaphore_wait(barrier, count)


def subsets(bits):
    out = [0]
    for b in bits:
        out = out + [j | b for j in out]
    return out


def gather_kernel(n_dp, n_head, orders, *refs):
    parts = len(orders)
    n = n_dp * n_head
    src, dst = refs[:parts], refs[parts : 2 * parts]
    send_sem, recv_sem, own_sem = refs[2 * parts :]
    place = []
    for j in range(n):
        d, h = flipped(j, n_dp, n_head)
        place.append(d * n_head + h)

    def copy(p, j, b):
        here = src[p] if j == 0 else dst[p].at[place[j]]
        k = p * n + (j | b)
        return pltpu.make_async_remote_copy(
            src_ref=here,
            dst_ref=dst[p].at[place[j]],
            send_sem=send_sem.at[k],
            recv_sem=recv_sem.at[k],
            device_id=flipped(b, n_dp, n_head),
            device_id_type=pl.DeviceIdType.MESH,
        )

    def arrival(p, j):
        k = p * n + j
        return pltpu.make_async_remote_copy(
            src_ref=src[p],
            dst_ref=dst[p].at[place[j]],
            send_sem=send_sem.at[k],
            recv_sem=recv_sem.at[k],
            device_id=flipped(1, n_dp, n_head),
            device_id_type=pl.DeviceIdType.MESH,
        )

    own = [pltpu.make_async_copy(src[p], dst[p].at[place[0]], own_sem.at[p]) for p in range(parts)]
    for o in own:
        o.start()
    greet(n, n_dp, n_head)
    started = []

    def start(p, j, b):
        c = copy(p, j, b)
        c.start()
        started.append(c)

    for step in range(len(orders[0]) + 1):
        for p in range(parts):
            order = orders[p]
            fresh = [0] if step == 0 else [j | order[step - 1] for j in subsets(order[: step - 1])]
            if step == 0:
                start(p, 0, order[0])
                start(p, 0, 1)
                continue
            old = subsets(order[: step - 1])
            if step < len(order):
                for j in old:
                    start(p, j, order[step])
            for j in fresh:
                arrival(p, j).wait_recv()
                if step < len(order):
                    start(p, j, order[step])
                start(p, j, 1)
    for p in range(parts):
        for j in subsets(orders[p]):
            arrival(p, j | 1).wait_recv()
    for c in started:
        c.wait_send()
    for o in own:
        o.wait()


def gather_all(arrays, n_dp, n_head):
    n = n_dp * n_head
    parts = len(arrays)
    any_ = pl.BlockSpec(memory_space=pl.ANY)
    vmem = pl.BlockSpec(memory_space=pltpu.VMEM)
    return pl.pallas_call(
        functools.partial(gather_kernel, n_dp, n_head, link_orders(n)[:parts]),
        out_shape=[jax.ShapeDtypeStruct((n,) + a.shape, a.dtype) for a in arrays],
        in_specs=[vmem] * parts,
        out_specs=[any_] * parts,
        scratch_shapes=[
            pltpu.SemaphoreType.DMA((parts * n,)),
            pltpu.SemaphoreType.DMA((parts * n,)),
            pltpu.SemaphoreType.DMA((parts,)),
        ],
        compiler_params=pltpu.CompilerParams(collective_id=0, has_side_effects=True),
    )(*arrays)


def scatter_kernel(n_dp, n_head, orders, *refs):
    parts = len(orders)
    n = n_dp * n_head
    half = n // 2
    src, out = refs[:parts], refs[parts : 2 * parts]
    acc, core, link = (refs[(2 + i) * parts : (3 + i) * parts] for i in range(3))
    core_send, core_recv, link_send, link_recv, own_sem = refs[5 * parts :]
    sib = flipped(1, n_dp, n_head)
    kinds = pl.DeviceIdType.MESH

    def place(j):
        d, h = flipped(j, n_dp, n_head)
        return d * n_head + h

    own, core_copy, link_copy = {}, {}, {}
    for p in range(parts):
        for j in subsets(orders[p][::-1])[::-1]:
            k = p * half + j // 2
            own[p, j] = pltpu.make_async_copy(src[p].at[place(j)], acc[p].at[j // 2], own_sem.at[k])
            core_copy[p, j] = pltpu.make_async_remote_copy(
                src_ref=src[p].at[place(j | 1)],
                dst_ref=core[p].at[j // 2],
                send_sem=core_send.at[k],
                recv_sem=core_recv.at[k],
                device_id=sib,
                device_id_type=kinds,
            )
    for c in own.values():
        c.start()
    greet(n, n_dp, n_head)

    def first_of(p):
        order = orders[p][::-1]
        return sorted(subsets(order), key=lambda j: [0 if j & b else 1 for b in order])

    for i in range(half):
        for p in range(parts):
            core_copy[p, first_of(p)[i]].start()

    def add(into, a, b):
        rows = a.shape[0]
        step = 16 if rows % 16 == 0 else rows
        kind = into.dtype

        def one(i, carry):
            r = pl.ds(pl.multiple_of(i * step, step), step)
            into[r, :] = (a[r, :].astype(F32) + b[r, :].astype(F32)).astype(kind)
            return carry

        lax.fori_loop(0, rows // step, one, 0)

    def send(p, j, b):
        k = p * half + j // 2
        c = pltpu.make_async_remote_copy(
            src_ref=acc[p].at[j // 2],
            dst_ref=link[p].at[j // 2],
            send_sem=link_send.at[k],
            recv_sem=link_recv.at[k],
            device_id=flipped(b, n_dp, n_head),
            device_id_type=kinds,
        )
        c.start()
        link_copy[p, j] = c

    steps = len(orders[0])

    def meet(p, j):
        core_copy[p, j].wait_recv()
        own[p, j].wait()
        add(acc[p].at[j // 2], acc[p].at[j // 2], core[p].at[j // 2])

    for p in range(parts):
        b = orders[p][steps - 1]
        for j in first_of(p):
            if j & b:
                meet(p, j)
                send(p, j, b)
    for p in range(parts):
        b = orders[p][steps - 1]
        for j in first_of(p):
            if not j & b:
                meet(p, j)
    for t in range(steps - 1, -1, -1):
        for p in range(parts):
            b = orders[p][t]
            left = [j for j in first_of(p) if not any(j & c for c in orders[p][t:])]
            for j in left:
                link_copy[p, j | b].wait_recv()
                into = out[p] if t == 0 else acc[p].at[j // 2]
                add(into, acc[p].at[j // 2], link[p].at[(j | b) // 2])
                if t > 0 and j & orders[p][t - 1]:
                    send(p, j, orders[p][t - 1])
    for c in core_copy.values():
        c.wait_send()
    for c in link_copy.values():
        c.wait_send()


def scatter_all(arrays, n_dp, n_head):
    n = n_dp * n_head
    half = n // 2
    parts = len(arrays)
    any_ = pl.BlockSpec(memory_space=pl.ANY)
    vmem = pl.BlockSpec(memory_space=pltpu.VMEM)
    slots = [pltpu.VMEM((half,) + a.shape[1:], a.dtype) for a in arrays]
    return pl.pallas_call(
        functools.partial(scatter_kernel, n_dp, n_head, link_orders(n)[:parts]),
        out_shape=[jax.ShapeDtypeStruct(a.shape[1:], F32) for a in arrays],
        in_specs=[any_] * parts,
        out_specs=[vmem] * parts,
        scratch_shapes=slots * 3 + [pltpu.SemaphoreType.DMA((parts * half,))] * 5,
        compiler_params=pltpu.CompilerParams(
            collective_id=1, has_side_effects=True, vmem_limit_bytes=48 * 1024 * 1024
        ),
    )(*arrays)


SMALL_ROWS = 8


def body(tokens, cotangent, bucket_ids, seq_lengths, *params):
    rows = tokens.shape[1]
    assert rows % LONGEST == 0
    mask = local_mask(bucket_ids, seq_lengths, rows)
    n_dp, n_head = lax.axis_size("dp"), lax.axis_size("head")
    if n_dp * n_head == 32:
        return kernel_body(tokens, cotangent, mask, n_dp, n_head, *params)
    return native_body(tokens, cotangent, mask, *params)


def kernel_body(tokens, cotangent, mask, n_dp, n_head, wq, qb, wk, wv, vb, wo, ob, g1, s1, wi, ib, wu, ub, g2, s2):
    n = n_dp * n_head
    width = wu.shape[1]
    r, c = wq.shape
    qkv_rows = 3 * r * c // width
    lanes = 128
    small = (qb, vb, ob, g1, s1, ib, ub, g2, s2)
    sizes = [a.size for a in small]
    flat = jnp.concatenate([a.reshape(-1).astype(F32) for a in small])
    pad = SMALL_ROWS * lanes - flat.size
    flat = jnp.pad(flat, (0, pad)).reshape(SMALL_ROWS, lanes)
    third = jnp.concatenate([jnp.stack([wq, wk, wv]).reshape(qkv_rows, width), wo], axis=0)
    gi_, gu_, gt_, gs_ = gather_all([wi.reshape(-1, width), wu, third, flat], n_dp, n_head)
    wi_ = gi_.reshape(-1, wi.shape[1])
    wu_ = gu_.reshape(-1, width)
    wqkv = gt_[:, :qkv_rows].reshape(n_dp, n_head, 3, r, c).transpose(2, 0, 3, 1, 4).reshape(3, n_dp * r, n_head * c)
    wo_ = gt_[:, qkv_rows:].reshape(-1, width)
    gs_ = gs_.reshape(n, -1)
    pieces = []
    at = 0
    for a, size in zip(small, sizes):
        piece = gs_[:, at : at + size]
        at += size
        if a.ndim == 2:
            piece = piece.reshape(n_dp, n_head, *a.shape).transpose(1, 2, 0, 3)
        pieces.append(piece.reshape(-1))
    qb_, vb_, ob_, g1_, s1_, ib_, ub_, g2_, s2_ = pieces
    p = (wqkv[0], qb_, wqkv[1], wqkv[2], vb_, wo_, ob_, g1_, s1_, wi_, ib_, wu_, ub_, g2_, s2_)
    out, g_in, big, s = layer(tokens, cotangent, mask, p)
    gqkv = jnp.stack([b.astype(BF16) for b in big[:3]])
    gqkv = gqkv.reshape(3, n_dp, r, n_head, c).transpose(1, 3, 0, 2, 4).reshape(n, qkv_rows, width)
    go, gi, gu = (b.astype(BF16) for b in big[3:])
    third = jnp.concatenate([gqkv, go.reshape(n, -1, width)], axis=1)
    order = (s[0], s[1], s[2], s[3], s[4], s[5], s[6], s[7], s[8])
    flat = []
    for a, g in zip(small, order):
        if a.ndim == 2:
            h, k = a.shape
            g = g.reshape(n_head, h, n_dp, k).transpose(2, 0, 1, 3)
        flat.append(g.reshape(n, -1))
    flat = jnp.pad(jnp.concatenate(flat, axis=1), ((0, 0), (0, pad))).reshape(n, SMALL_ROWS, lanes)
    gi, gu, third, flat = scatter_all(
        [gi.reshape(n, -1, width), gu.reshape(n, -1, width), third, flat], n_dp, n_head
    )
    gqkv = third[:qkv_rows].reshape(3, r, c)
    flat = flat.reshape(-1)
    pieces = []
    at = 0
    for a, size in zip(small, sizes):
        pieces.append(flat[at : at + size].reshape(a.shape))
        at += size
    gqb, gvb, gob, gg1, gs1, gib, gub, gg2, gs2 = pieces
    return (out, g_in, gqkv[0], gqb, gqkv[1], gqkv[2], gvb, third[qkv_rows:], gob, gg1, gs1, gi.reshape(wi.shape), gib, gu, gub, gg2, gs2)


def native_body(tokens, cotangent, mask, wq, qb, wk, wv, vb, wo, ob, g1, s1, wi, ib, wu, ub, g2, s2):
    both = ("dp", "head")
    ag = lambda a, ax, dim: lax.all_gather(a, ax, axis=dim, tiled=True)
    wqkv = ag(jnp.stack([wq, wk, wv]), "dp", 1)
    wqkv = ag(wqkv, "head", 2)
    ob_, g1_, s1_, ub_, g2_, s2_, ib_ = (ag(a, both, 0) for a in (ob, g1, s1, ub, g2, s2, ib))
    qb_, vb_ = (ag(ag(a, "dp", 1), "head", 0) for a in (qb, vb))
    p = (wqkv[0], qb_, wqkv[1], wqkv[2], vb_, ag(wo, both, 0), ob_, g1_, s1_, ag(wi, both, 0), ib_, ag(wu, both, 0), ub_, g2_, s2_)
    out, g_in, big, small = layer(tokens, cotangent, mask, p)
    sc = lambda a, ax, dim: lax.psum_scatter(a, ax, scatter_dimension=dim, tiled=True)
    gqkv = jnp.stack([b.astype(BF16) for b in big[:3]])
    gqkv = sc(sc(gqkv, "head", 2), "dp", 1).astype(F32)
    go, gi, gu = (sc(b.astype(BF16), both, 0).astype(F32) for b in big[3:])
    hb = lambda a: sc(sc(a.reshape(-1, HD), "head", 0), "dp", 1)
    s = small
    return (out, g_in, gqkv[0], hb(s[0]), gqkv[1], gqkv[2], hb(s[1]), go, sc(s[2], both, 0), sc(s[3], both, 0), sc(s[4], both, 0), gi, sc(s[5], both, 0), gu, sc(s[6], both, 0), sc(s[7], both, 0), sc(s[8], both, 0))


def solution(mesh):
    rows = P(None, ("dp", "head"), None)
    dense = P(("dp", "head"), None)
    flat = P(("dp", "head"))
    tile = P("dp", "head")
    bias = P("head", "dp")
    params = (tile, bias, tile, tile, bias, dense, flat, flat, flat, dense, flat, dense, flat, flat, flat)
    return jax.shard_map(
        body,
        mesh=mesh,
        in_specs=(rows, rows, P(None, "dp"), P(None, "dp", None)) + params,
        out_specs=(rows, rows) + params,
        check_vma=False,
    )
```
